512 devices in a mesh: dp: 128 (over y, z, core), mp: 4 (over x).
Axes of the slice: x: 4, y: 4, z: 16, core: 2. Of those that a mesh axis runs over, the one named last changes fastest.
Arguments:
- hidden: bfloat16 [90112, 7168], P('dp', 'mp'), may hold values from -0.1875 to 0.1875
- router_weight: bfloat16 [7168, 256], P(('mp', 'dp')), may hold values from -3 to 3
- logits: float32 [90112, 256], P(('dp', 'mp')), may hold values from -12 to 240
- first_pot: float32 [256], replicated, may hold values from -1 to 1
- second_pot: float32 [256], replicated, may hold values from -1 to 1
- expert_index: int32 [90112], P(('dp', 'mp')), may hold values from 0 to 255
- loss_grad: float32 [90112], P(('dp', 'mp')), may hold values from -9 to 9
Outputs:
- weight_grad: float32 [7168, 256], P(('mp', 'dp'))
- hidden_grad: bfloat16 [90112, 7168], P('dp', 'mp')
The draws below stay inside these ranges and needn't reach their ends.
All inputs are finite; a program needn't handle non-finite values.
Results may differ from the reference program's by a relative error of at most 0.005.
Values may be sent and summed in bfloat16 or wider, within the bound.
No kernel may reach another device: no remote copies, remote signals or barrier semaphores. Data moves between devices by JAX's collectives and lax.ppermute only.
A program may use at most 64 MiB of HBM per device.

```python
import jax
import jax.numpy as jnp
from jax import lax

D = 7168
E = 256
TOK_DEV = 704
TOKENS = 90112


def draw_logits(key, part):
    second_key = jax.random.fold_in(jax.random.fold_in(key, 11), 1)
    base = jax.random.normal(second_key, (TOKENS, E), jnp.float32) * 2.0
    return jnp.clip(base, -8.0, 8.0)


def draw_loss_grad(key, part):
    first_key, second_key, third_key = jax.random.split(jax.random.fold_in(key, 23), 3)
    blocks = TOKENS // TOK_DEV
    scales = jnp.exp(jax.random.uniform(first_key, (blocks, 1), jnp.float32, -3.0, 1.0986))
    common_sign = jnp.where(jax.random.bernoulli(second_key, 0.5, ()), 1.0, -1.0)
    noise = jnp.clip(jax.random.normal(third_key, (blocks, TOK_DEV), jnp.float32) * 0.5, -2.0, 2.0)
    return (scales * (0.7 * common_sign + noise)).reshape(TOKENS)


def with_ends(array, stream_key, smallest, high):
    longest = array.shape.index(max(array.shape))
    spots = []
    for shift in (0, 1):
        where = [jax.random.randint(jax.random.fold_in(stream_key, axis), (), 0, length) for axis, length in enumerate(array.shape)]
        where[longest] = (where[longest] + shift) % array.shape[longest]
        spots.append(tuple(where))
    return array.at[spots[0]].set(smallest).at[spots[1]].set(high)


def level_of(rng, dims, pieces, least, high):
    def one(dim, parts):
        steps = jax.random.uniform(jax.random.fold_in(jax.random.fold_in(rng, 6), dim), (parts,), jnp.float32, least / len(pieces), high / len(pieces))
        return jnp.repeat(jnp.exp(steps), dims[dim] // parts).reshape((-1,) + (1,) * (len(dims) - dim - 1))

    gain = one(*pieces[0])
    for cut in pieces[1:]:
        gain = gain * one(*cut)
    return gain


def centred(key, shape, width, limit, cuts=(), kind=jnp.bfloat16):
    level = level_of(key, shape, cuts, -0.22, 0.18) if cuts else 1.0
    drawn = jax.random.normal(key, shape, jnp.float32) * width * level
    return jnp.minimum(jnp.maximum(drawn, -limit), limit).astype(kind)


def setup_inputs(seed: int = 0) -> dict:
    seeds = jax.random.split(jax.random.key(seed), 8)
    return {
        "hidden": centred(seeds[0], (TOKENS, D), 0.03, 0.1875, ((0, 128), (1, 4))),
        "router_weight": centred(seeds[1], (D, E), 0.5, 3.0, ((0, 512),)),
        "logits": draw_logits(jax.random.fold_in(seeds[7], 71), 0),
        "first_pot": jnp.clip(jax.random.uniform(seeds[3], (E,), jnp.float32, -1.0, 1.0), -1.0, 1.0),
        "second_pot": jnp.clip(jax.random.uniform(seeds[4], (E,), jnp.float32, -1.0, 1.0), -1.0, 1.0),
        "expert_index": with_ends(jax.random.randint(seeds[5], (TOKENS,), 0, E), jax.random.fold_in(seeds[5], 1), 0, E - 1).astype(jnp.int32),
        "loss_grad": draw_loss_grad(jax.random.fold_in(seeds[7], 71), 0),
    }


def neg_lse(values):
    top = jnp.max(values, axis=1, keepdims=True)
    return -(top[:, 0] + jnp.log(jnp.sum(jnp.exp(values - top), axis=1)))


def reference(hidden, router_weight, logits, first_pot, second_pot, expert_index, loss_grad):
    ratio = E / TOKENS
    first_row = neg_lse(logits)
    first_soft = jnp.exp(logits + first_row[:, None])
    shifted = logits + first_pot[None, :]
    second_row = neg_lse(shifted)
    second_soft = jnp.exp(shifted + second_row[:, None])
    first_col = ratio * jnp.exp(logits + first_row[:, None] + first_pot[None, :])
    prob = jnp.exp(logits + second_row[:, None] + second_pot[None, :])
    second_col = ratio * prob
    onehot = (expert_index[:, None] == jnp.arange(E, dtype=jnp.int32)[None, :]).astype(jnp.float32)
    direct = onehot * prob * loss_grad[:, None]
    second_colgrad = jnp.sum(direct, axis=0)
    second_rowgrad = jnp.sum(direct, axis=1) - jnp.dot(second_col, second_colgrad, precision=lax.Precision.HIGHEST)
    first_colgrad = -jnp.sum(second_rowgrad[:, None] * second_soft, axis=0)
    first_rowgrad = -jnp.dot(first_col, first_colgrad, precision=lax.Precision.HIGHEST)
    score_grad = (direct - second_colgrad[None, :] * second_col - second_rowgrad[:, None] * second_soft
                  - first_colgrad[None, :] * first_col - first_rowgrad[:, None] * first_soft).astype(jnp.bfloat16)
    weight_grad = jnp.dot(hidden.T, score_grad, preferred_element_type=jnp.float32)
    hidden_grad = jnp.dot(score_grad, router_weight.T, preferred_element_type=jnp.float32).astype(jnp.bfloat16)
    return weight_grad, hidden_grad
```

```python
import functools

import jax
import jax.numpy as jnp
from jax import lax
from jax.experimental import pallas as pl
from jax.experimental.pallas import tpu as pltpu
from jax.sharding import Mesh
from jax.sharding import PartitionSpec as P

DP = ("y", "z", "c")
F32 = jnp.float32
BF16 = jnp.bfloat16
PAD = 16


def to_each(array, axes):
    devices = lax.axis_size(axes)
    return lax.all_to_all(
        jnp.broadcast_to(array[None], (devices, *array.shape)), axes, 0, 0, tiled=True
    )


def call(kernel, out_shape, *args, flops=0, nbytes=0, name=None, **kwargs):
    return pl.pallas_call(
        kernel,
        out_shape=out_shape,
        cost_estimate=pl.CostEstimate(flops=flops, transcendentals=0, bytes_accessed=nbytes),
        name=name,
        **kwargs,
    )(*args)


def split_two(value):
    high = value.astype(BF16)
    low = (value - high.astype(F32)).astype(BF16)
    return high.astype(F32), low.astype(F32)


def as_column(row, tokens):
    shape = (tokens, row.shape[1])
    same = lax.broadcasted_iota(jnp.int32, shape, 0) == lax.broadcasted_iota(jnp.int32, shape, 1)
    return jnp.sum(jnp.where(same, row, 0.0), axis=1, keepdims=True)


def exponent_kernel(logits_ref, index_ref, grad_ref, out_ref):
    tokens, experts = logits_ref.shape
    logits = logits_ref[...]
    weight = jnp.exp(logits - jnp.max(logits, axis=1, keepdims=True))
    index = as_column(index_ref[...].astype(F32), tokens)
    lane = lax.broadcasted_iota(jnp.int32, (tokens, experts), 1).astype(F32)
    out_ref[:tokens, :] = jnp.where(lane == index, -weight, weight).astype(BF16)
    high, low = split_two(grad_ref[...])
    rows = out_ref.shape[0] - tokens
    row = lax.broadcasted_iota(jnp.int32, (rows, experts), 0)
    tail = jnp.where(row == 0, high, jnp.where(row == 1, low, 0.0))
    out_ref[tokens:, :] = tail.astype(BF16)


def tokens_of(gathered_ref, first_pot, second_pot, block, tokens):
    signed = gathered_ref[block, :tokens, :].astype(F32)
    tail = gathered_ref[block, tokens:, :].astype(F32)
    grad = as_column(tail[0:1, :] + tail[1:2, :], tokens)
    weight = jnp.abs(signed)
    first_gain = jnp.exp(first_pot)
    second_gain = jnp.exp(second_pot)
    first_scale = 1.0 / jnp.sum(weight, axis=1, keepdims=True)
    second_scale = 1.0 / jnp.sum(weight * first_gain, axis=1, keepdims=True)
    hot = jnp.where(signed < 0.0, grad, 0.0)
    return weight, first_gain, second_gain, first_scale, second_scale, hot


def direct_kernel(gathered_ref, first_ref, second_ref, router_ref, out_ref, *, tokens):
    total = 0.0
    for block in range(gathered_ref.shape[0]):
        weight, _, second_gain, _, second_scale, hot = tokens_of(
            gathered_ref, first_ref[...], second_ref[...], block, tokens
        )
        total = total + jnp.sum(weight * hot * second_scale, axis=0, keepdims=True) * second_gain
    high, low = split_two(total)
    rows, experts = router_ref.shape
    row = lax.broadcasted_iota(jnp.int32, (PAD, experts), 0)
    out_ref[:rows, :] = router_ref[...]
    out_ref[rows : rows + 1, :] = high.astype(BF16)
    out_ref[rows + 1 : rows + 2, :] = low.astype(BF16)


def along_kernel(parts_ref, out_ref, *, rows):
    members = parts_ref.shape[0]
    pair = parts_ref[:, rows : rows + 2, :].astype(F32)
    total = jnp.sum(jnp.sum(pair, axis=0), axis=0, keepdims=True)
    high, low = split_two(total)
    for member in range(1, members):
        out_ref[member * PAD : (member + 1) * PAD, :] = parts_ref[member]
    block = parts_ref[0].astype(F32)
    row = lax.broadcasted_iota(jnp.int32, block.shape, 0)
    block = jnp.where(row == rows, high, jnp.where(row == rows + 1, low, block))
    out_ref[0:PAD, :] = block.astype(BF16)


def across_kernel(parts_ref, out_ref, *, rows):
    total = 0.0
    for member in range(parts_ref.shape[0]):
        block = parts_ref[member, 0:PAD, :].astype(F32)
        total = total + jnp.sum(block[rows : rows + 2, :], axis=0, keepdims=True)
    out_ref[...] = total


def second_row_grad(token_parts, col_grad, ratio):
    weight, _, second_gain, _, second_scale, hot = token_parts
    inner = second_gain * (hot - ratio * col_grad)
    return jnp.sum(weight * inner, axis=1, keepdims=True) * second_scale, inner


def first_col_kernel(gathered_ref, first_ref, second_ref, sums_ref, out_ref, *, tokens, ratio):
    col_grad = jnp.sum(sums_ref[...], axis=0)
    total = 0.0
    for block in range(gathered_ref.shape[0]):
        parts = tokens_of(gathered_ref, first_ref[...], second_ref[...], block, tokens)
        row_grad, _ = second_row_grad(parts, col_grad, ratio)
        weight, first_gain, _, _, second_scale, _ = parts
        total = total - jnp.sum(weight * (row_grad * second_scale), axis=0, keepdims=True) * first_gain
    out_ref[...] = total


def score_kernel(
    gathered_ref,
    first_ref,
    second_ref,
    sums_ref,
    first_col_ref,
    hidden_ref,
    score_ref,
    out_ref,
    *,
    tokens,
    ratio,
):
    col_grad = jnp.sum(sums_ref[...], axis=0)
    first_col = first_col_ref[...]
    for block in range(gathered_ref.shape[0]):
        parts = tokens_of(gathered_ref, first_ref[...], second_ref[...], block, tokens)
        row_grad, inner = second_row_grad(parts, col_grad, ratio)
        weight, first_gain, _, first_scale, second_scale, _ = parts
        scaled = ratio * first_gain * first_col
        first_row = -jnp.sum(weight * scaled, axis=1, keepdims=True) * first_scale
        score = weight * (
            second_scale * (inner - first_gain * row_grad) - first_scale * (scaled + first_row)
        )
        score_ref[block * tokens : (block + 1) * tokens, :] = score.astype(BF16)
    score = score_ref[...]
    size = out_ref.shape[1]
    for part in range(out_ref.shape[0]):
        out_ref[part] = jnp.dot(
            hidden_ref[part * size : (part + 1) * size, :], score, preferred_element_type=F32
        ).astype(BF16)


def whole_part(value, size):
    return jnp.floor((value + 0.5) * (1.0 / size))


def transpose_kernel(hidden_ref, out_ref, *, along, rows):
    size = hidden_ref.shape[1]
    target = lax.broadcasted_iota(jnp.int32, (size, size), 0).astype(F32)
    source = lax.broadcasted_iota(jnp.int32, (size, size), 1).astype(F32)
    span = along * rows
    outer = whole_part(target, 2 * span)
    rest = target - outer * (2 * span)
    core = whole_part(rest, span)
    rest = rest - core * span
    place = whole_part(rest, rows)
    wanted = outer * (2 * span) + place * (2 * rows) + core * rows + (rest - place * rows)
    order = jnp.where(source == wanted, 1.0, 0.0).astype(BF16)
    out_ref[...] = lax.dot_general(
        order, hidden_ref[...], (((1,), (1,)), ((), ())), preferred_element_type=F32
    ).astype(BF16)


def near_kernel(parts_ref, out_ref, *, along, rows):
    total = 0.0
    for member in range(parts_ref.shape[0]):
        total = total + parts_ref[member].astype(F32)
    for place in range(along):
        out_ref[place] = total[place * rows : (place + 1) * rows, :].astype(BF16)


def far_kernel(parts_ref, out_ref):
    total = 0.0
    for member in range(parts_ref.shape[0]):
        total = total + parts_ref[member].astype(F32)
    out_ref[...] = total


def hidden_kernel(core_ref, score_ref, mine_ref, other_ref, out_ref, router_ref, *, rows):
    members, padded, _ = mine_ref.shape
    along = padded // PAD
    size = 2 * along * rows

    @pl.when(pl.program_id(0) == 0)
    def _():
        target = lax.broadcasted_iota(jnp.int32, (size, padded), 0).astype(F32)
        column = lax.broadcasted_iota(jnp.int32, (size, padded), 1).astype(F32)
        place = whole_part(column, PAD)
        row = column - place * PAD
        base = place * (2 * rows) + row
        kept = row < rows
        mine_at = core_ref[0].astype(F32) * rows
        mine = jnp.where(kept & (target == base + mine_at), 1.0, 0.0).astype(BF16)
        other = jnp.where(kept & (target == base + (rows - mine_at)), 1.0, 0.0).astype(BF16)
        for member in range(members):
            whole = jnp.dot(mine, mine_ref[member], preferred_element_type=F32) + jnp.dot(
                other, other_ref[member], preferred_element_type=F32
            )
            router_ref[member * size : (member + 1) * size, :] = whole.astype(BF16)

    width = out_ref.shape[1]
    start = pl.multiple_of(pl.program_id(0) * width, width)
    out_ref[...] = lax.dot_general(
        score_ref[...],
        router_ref[pl.ds(start, width), :],
        (((1,), (1,)), ((), ())),
        preferred_element_type=F32,
    ).astype(BF16)


def body(hidden, router_weight, logits, first_pot, second_pot, expert_index, loss_grad):
    tokens, experts = logits.shape
    rows = router_weight.shape[0]
    across, along = lax.axis_size("y"), lax.axis_size("z")
    blocks = lax.axis_size("x")
    ratio = experts / (tokens * blocks * lax.axis_size(DP))
    all_tokens, width = hidden.shape
    vmem = pl.BlockSpec(memory_space=pltpu.VMEM)

    padding = ((0, 0), (0, experts - tokens))
    exponents = call(
        exponent_kernel,
        jax.ShapeDtypeStruct((tokens + PAD, experts), BF16),
        logits,
        jnp.pad(expert_index[None], padding),
        jnp.pad(loss_grad[None], padding),
        name="exponents",
    )
    gathered = to_each(exponents, "x")
    pots = (first_pot[None], second_pot[None])

    half = across * along * 2 * rows // max(across // 2, 1)
    transposed = call(
        functools.partial(transpose_kernel, along=along, rows=rows),
        jax.ShapeDtypeStruct((width, all_tokens), BF16),
        hidden,
        grid=(width // half,),
        in_specs=[pl.BlockSpec((all_tokens, half), lambda i: (0, i))],
        out_specs=pl.BlockSpec((half, all_tokens), lambda i: (i, 0)),
        flops=2 * width * half * all_tokens,
        nbytes=4 * width * all_tokens,
        name="transposed",
    )

    sent = call(
        functools.partial(direct_kernel, tokens=tokens),
        jax.ShapeDtypeStruct((PAD, experts), BF16),
        gathered,
        *pots,
        router_weight,
        name="direct",
    )
    along_parts = to_each(sent, "z")
    sent = call(
        functools.partial(along_kernel, rows=rows),
        jax.ShapeDtypeStruct((along * PAD, experts), BF16),
        along_parts,
        name="along",
    )
    across_parts = to_each(sent, "y")
    sent = call(
        functools.partial(across_kernel, rows=rows),
        jax.ShapeDtypeStruct((1, experts), F32),
        across_parts,
        name="across",
    )
    sums = to_each(sent, "c")
    other_router = lax.ppermute(across_parts, "c", [(0, 1), (1, 0)])

    partial_col = call(
        functools.partial(first_col_kernel, tokens=tokens, ratio=ratio),
        jax.ShapeDtypeStruct((1, experts), F32),
        gathered,
        *pots,
        sums,
        name="first_col",
    )
    first_col = jnp.sum(to_each(partial_col, DP), axis=0)

    score, products = call(
        functools.partial(score_kernel, tokens=tokens, ratio=ratio),
        (
            jax.ShapeDtypeStruct((all_tokens, experts), BF16),
            jax.ShapeDtypeStruct((2 * across, along * rows, experts), BF16),
        ),
        gathered,
        *pots,
        sums,
        first_col,
        transposed,
        flops=2 * all_tokens * width * experts,
        nbytes=2 * all_tokens * width,
        name="score",
    )
    near = lax.all_to_all(products, ("y", "c"), 0, 0, tiled=True)
    far = call(
        functools.partial(near_kernel, along=along, rows=rows),
        jax.ShapeDtypeStruct((along, rows, experts), BF16),
        near,
        name="near",
    )
    far = lax.all_to_all(far, "z", 0, 0, tiled=True)

    chunk = 256 if width % 256 == 0 else width
    hidden_grad = call(
        functools.partial(hidden_kernel, rows=rows),
        jax.ShapeDtypeStruct((all_tokens, width), BF16),
        lax.axis_index("c").astype(jnp.int32)[None],
        score,
        across_parts,
        other_router,
        grid=(width // chunk,),
        in_specs=[
            pl.BlockSpec(memory_space=pltpu.SMEM),
            vmem,
            vmem,
            vmem,
        ],
        out_specs=pl.BlockSpec((all_tokens, chunk), lambda i: (0, i)),
        scratch_shapes=[pltpu.VMEM((width, experts), BF16)],
        flops=2 * all_tokens * width * experts,
        nbytes=2 * all_tokens * width,
        name="hidden_grad",
    )
    weight_grad = call(
        far_kernel, jax.ShapeDtypeStruct((rows, experts), F32), far, name="weight_grad"
    )
    return weight_grad, hidden_grad


def solution(mesh):
    dp, mp = mesh.devices.shape
    along = dp // 8
    split = Mesh(mesh.devices.reshape(4, along, 2, mp), ("y", "z", "c", "x"))
    token_rows = ("y", "z", "c", "x")
    weight_rows = ("x", "y", "z", "c")
    return jax.shard_map(
        body,
        mesh=split,
        in_specs=(
            P(DP, "x"),
            P(weight_rows, None),
            P(token_rows, None),
            P(),
            P(),
            P(token_rows),
            P(token_rows),
        ),
        out_specs=(P(weight_rows, None), P(DP, "x")),
        check_vma=False,
    )
```

```python
import functools

import jax
import jax.numpy as jnp
from jax import lax
from jax.experimental import pallas as pl
from jax.experimental.pallas import tpu as pltpu
from jax.sharding import Mesh
from jax.sharding import PartitionSpec as P

DP = ("y", "z", "c")
F32 = jnp.float32
BF16 = jnp.bfloat16
PAD = 16


def kept(shape, dtype):
    return pltpu.VMEM(shape, dtype)


def placed(array, near):
    return pltpu.with_memory_space_constraint(array, pltpu.VMEM if near else pltpu.HBM)


def call(kernel, shapes, *args, far=(), flops=0, nbytes=0, limit=16, name=None, **kwargs):
    return pl.pallas_call(
        kernel,
        out_shape=shapes,
        cost_estimate=pl.CostEstimate(flops=flops, transcendentals=0, bytes_accessed=nbytes),
        name=name,
        compiler_params=pltpu.CompilerParams(vmem_limit_bytes=limit << 20),
        **kwargs,
    )(*(placed(arg, at not in far) for at, arg in enumerate(args)))


def split_two(value):
    high = value.astype(BF16)
    low = (value - high.astype(F32)).astype(BF16)
    return high.astype(F32), low.astype(F32)


def as_column(row, tokens):
    shape = (tokens, row.shape[1])
    same = lax.broadcasted_iota(jnp.int32, shape, 0) == lax.broadcasted_iota(jnp.int32, shape, 1)
    return jnp.sum(jnp.where(same, row, 0.0), axis=1, keepdims=True)


def exponent_kernel(
    logits_ref, index_ref, grad_ref, first_ref, second_ref, router_ref, out_ref, gains_ref, copy_ref
):
    tokens, experts = logits_ref.shape
    logits = logits_ref[...]
    weight = jnp.exp(logits - jnp.max(logits, axis=1, keepdims=True))
    index = as_column(index_ref[...].astype(F32), tokens)
    lane = lax.broadcasted_iota(jnp.int32, (tokens, experts), 1).astype(F32)
    out_ref[:tokens, :] = jnp.where(lane == index, -weight, weight).astype(BF16)
    high, low = split_two(grad_ref[...])
    rows = out_ref.shape[0] - tokens
    out_ref[tokens:, :] = jnp.zeros((rows, experts), BF16)
    row = lax.broadcasted_iota(jnp.int32, (rows, tokens), 0)
    tail = jnp.where(row == 0, high, jnp.where(row == 1, low, 0.0))
    out_ref[tokens:, :tokens] = tail.astype(BF16)
    gains_ref[0:1, :] = jnp.exp(first_ref[...])
    gains_ref[1:2, :] = jnp.exp(second_ref[...])
    copy_ref[...] = router_ref[...]


def tokens_of(gathered_ref, gains_ref, block, tokens):
    signed = gathered_ref[block, :tokens, :].astype(F32)
    tail = gathered_ref[block, tokens:, :].astype(F32)
    grad = as_column(tail[0:1, :] + tail[1:2, :], tokens)
    weight = jnp.abs(signed)
    second_scale = 1.0 / jnp.sum(weight * gains_ref[0:1, :], axis=1, keepdims=True)
    hot = jnp.where(signed < 0.0, grad, 0.0)
    return weight, second_scale, hot


def direct_kernel(gathered_ref, gains_ref, router_ref, out_ref, *, tokens):
    total = 0.0
    for block in range(gathered_ref.shape[0]):
        weight, second_scale, hot = tokens_of(gathered_ref, gains_ref, block, tokens)
        total = total + jnp.sum(weight * hot * second_scale, axis=0, keepdims=True)
    high, low = split_two(total * gains_ref[1:2, :])
    rows = router_ref.shape[0]
    for member in range(out_ref.shape[0]):
        out_ref[member, :rows, :] = router_ref[...]
        out_ref[member, rows : rows + 1, :] = high.astype(BF16)
        out_ref[member, rows + 1 : rows + 2, :] = low.astype(BF16)


def prepare_kernel(gathered_ref, gains_ref, direct_ref, prob_ref, soft_ref, *, tokens):
    for block in range(gathered_ref.shape[0]):
        weight, second_scale, hot = tokens_of(gathered_ref, gains_ref, block, tokens)
        here = slice(block * tokens, (block + 1) * tokens)
        prob = weight * gains_ref[1:2, :] * second_scale
        prob_ref[here, :] = prob
        direct_ref[here, :] = prob * hot
        soft_ref[here, :] = weight * gains_ref[0:1, :] * second_scale


def along_kernel(parts_ref, out_ref, *, rows):
    members = parts_ref.shape[0]
    pair = parts_ref[:, rows : rows + 2, :].astype(F32)
    total = jnp.sum(jnp.sum(pair, axis=0), axis=0, keepdims=True)
    high, low = split_two(total)
    for member in range(1, members):
        out_ref[member * PAD : (member + 1) * PAD, :] = parts_ref[member]
    block = parts_ref[0].astype(F32)
    row = lax.broadcasted_iota(jnp.int32, block.shape, 0)
    block = jnp.where(row == rows, high, jnp.where(row == rows + 1, low, block))
    out_ref[0:PAD, :] = block.astype(BF16)


def across_kernel(parts_ref, out_ref, *, rows):
    total = 0.0
    for member in range(parts_ref.shape[0]):
        block = parts_ref[member, 0:PAD, :].astype(F32)
        total = total + jnp.sum(block[rows : rows + 2, :], axis=0, keepdims=True)
    out_ref[...] = total


def second_row_grad(direct, prob, scaled):
    return jnp.sum(direct - prob * scaled, axis=1, keepdims=True)


def first_col_kernel(direct_ref, prob_ref, soft_ref, sums_ref, out_ref, *, ratio):
    scaled = ratio * jnp.sum(sums_ref[...], axis=0)
    row_grad = second_row_grad(direct_ref[...], prob_ref[...], scaled)
    total = -jnp.sum(soft_ref[...] * row_grad, axis=0, keepdims=True)
    for member in range(out_ref.shape[0]):
        out_ref[member] = total


def second_kernel(gathered_ref, gains_ref, sums_ref, out_ref, first_ref, *, ratio, tokens):
    scaled = ratio * jnp.sum(sums_ref[...], axis=0)
    for block in range(gathered_ref.shape[0]):
        weight, second_scale, hot = tokens_of(gathered_ref, gains_ref, block, tokens)
        here = slice(block * tokens, (block + 1) * tokens)
        left = weight * second_scale * (gains_ref[1:2, :] * (hot - scaled))
        row = jnp.sum(left, axis=1, keepdims=True)
        out_ref[here, :] = left - weight * gains_ref[0:1, :] * (second_scale * row)
        first_ref[here, :] = weight * (1.0 / jnp.sum(weight, axis=1, keepdims=True))


def score_kernel(
    second_ref,
    first_ref,
    gains_ref,
    first_col_ref,
    hidden_ref,
    score_ref,
    out_ref,
    near_ref,
    done_ref,
    *,
    ratio,
):
    parts, size, _ = out_ref.shape
    copies = []
    for part in range(parts):
        here = pl.ds(part * size, size)
        copies.append(
            pltpu.make_async_copy(hidden_ref.at[here], near_ref.at[here], done_ref.at[part])
        )
        copies[part].start()
    scaled = ratio * gains_ref[0:1, :] * jnp.sum(first_col_ref[...], axis=0)
    first = first_ref[...]
    row = jnp.sum(first * scaled, axis=1, keepdims=True)
    score = (second_ref[...] - first * (scaled - row)).astype(BF16)
    score_ref[...] = score
    for part in range(parts):
        copies[part].wait()
        out_ref[part] = jnp.dot(
            near_ref[part * size : (part + 1) * size, :],
            score_ref[...],
            preferred_element_type=F32,
        ).astype(BF16)


def whole_part(value, size):
    return jnp.floor((value + 0.5) * (1.0 / size))


def transpose_kernel(hidden_ref, out_ref, *, along, rows):
    span = along * rows
    size = 4 * span if out_ref.shape[0] % (4 * span) == 0 else 2 * span
    target = lax.broadcasted_iota(jnp.int32, (size, size), 0).astype(F32)
    source = lax.broadcasted_iota(jnp.int32, (size, size), 1).astype(F32)
    outer = whole_part(target, 2 * span)
    rest = target - outer * (2 * span)
    core = whole_part(rest, span)
    rest = rest - core * span
    place = whole_part(rest, rows)
    wanted = outer * (2 * span) + place * (2 * rows) + core * rows + (rest - place * rows)
    order = jnp.where(source == wanted, 1.0, 0.0).astype(BF16)
    for start in range(0, out_ref.shape[0], size):
        out_ref[start : start + size, :] = lax.dot_general(
            order,
            hidden_ref[:, start : start + size],
            (((1,), (1,)), ((), ())),
            preferred_element_type=F32,
        ).astype(BF16)


def near_kernel(parts_ref, out_ref, *, along, rows):
    total = 0.0
    for member in range(parts_ref.shape[0]):
        total = total + parts_ref[member].astype(F32)
    for place in range(along):
        out_ref[place] = total[place * rows : (place + 1) * rows, :].astype(BF16)


def far_kernel(parts_ref, out_ref):
    total = 0.0
    for member in range(parts_ref.shape[0]):
        total = total + parts_ref[member].astype(F32)
    out_ref[...] = total


def hidden_kernel(core_ref, score_ref, mine_ref, other_ref, out_ref, router_ref, *, rows):
    members, padded, _ = mine_ref.shape
    along = padded // PAD
    size = 2 * along * rows

    @pl.when(pl.program_id(0) == 0)
    def _():
        target = lax.broadcasted_iota(jnp.int32, (size, padded), 0).astype(F32)
        column = lax.broadcasted_iota(jnp.int32, (size, padded), 1).astype(F32)
        place = whole_part(column, PAD)
        row = column - place * PAD
        base = place * (2 * rows) + row
        kept = row < rows
        mine_at = core_ref[0].astype(F32) * rows
        mine = jnp.where(kept & (target == base + mine_at), 1.0, 0.0).astype(BF16)
        other = jnp.where(kept & (target == base + (rows - mine_at)), 1.0, 0.0).astype(BF16)
        for member in range(members):
            whole = jnp.dot(mine, mine_ref[member], preferred_element_type=F32) + jnp.dot(
                other, other_ref[member], preferred_element_type=F32
            )
            router_ref[member * size : (member + 1) * size, :] = whole.astype(BF16)

    width = out_ref.shape[1]
    start = pl.multiple_of(pl.program_id(0) * width, width)
    out_ref[...] = lax.dot_general(
        score_ref[...],
        router_ref[pl.ds(start, width), :],
        (((1,), (1,)), ((), ())),
        preferred_element_type=F32,
    ).astype(BF16)


def body(hidden, router_weight, logits, first_pot, second_pot, expert_index, loss_grad):
    tokens, experts = logits.shape
    rows = router_weight.shape[0]
    across, along = lax.axis_size("y"), lax.axis_size("z")
    blocks = lax.axis_size("x")
    ratio = experts / (tokens * blocks * lax.axis_size(DP))
    all_tokens, width = hidden.shape
    vmem = pl.BlockSpec(memory_space=pltpu.VMEM)
    exponents, gains, router = call(
        exponent_kernel,
        (
            kept((tokens + PAD, experts), BF16),
            kept((2, experts), F32),
            kept((rows, experts), BF16),
        ),
        logits,
        expert_index[None],
        loss_grad[None],
        first_pot[None],
        second_pot[None],
        router_weight,
        far=range(6),
        name="exponents",
    )
    gathered = lax.all_gather(exponents, "x")
    whole = (all_tokens, experts)

    transposed = call(
        functools.partial(transpose_kernel, along=along, rows=rows),
        jax.ShapeDtypeStruct((width, all_tokens), BF16),
        hidden,
        far=(0,),
        in_specs=[vmem],
        out_specs=vmem,
        flops=width * width * all_tokens,
        nbytes=4 * width * all_tokens,
        limit=32,
        name="transposed",
    )

    sent = call(
        functools.partial(direct_kernel, tokens=tokens),
        jax.ShapeDtypeStruct((along, PAD, experts), BF16),
        gathered,
        gains,
        router,
        name="direct",
    )
    along_parts = lax.all_to_all(sent, "z", 0, 0, tiled=True)
    direct, prob, soft = call(
        functools.partial(prepare_kernel, tokens=tokens),
        (kept(whole, F32),) * 3,
        gathered,
        gains,
        flops=40 * all_tokens * experts,
        nbytes=14 * all_tokens * experts,
        name="prepared",
    )
    sent = call(
        functools.partial(along_kernel, rows=rows),
        kept((along * PAD, experts), BF16),
        along_parts,
        name="along",
    )
    across_parts = lax.all_gather(sent, "y")
    sent = call(
        functools.partial(across_kernel, rows=rows),
        kept((1, experts), F32),
        across_parts,
        name="across",
    )
    sums = lax.all_gather(sent, "c")
    other_router = lax.ppermute(across_parts, "c", [(0, 1), (1, 0)])

    partial_col = call(
        functools.partial(first_col_kernel, ratio=ratio),
        jax.ShapeDtypeStruct((lax.axis_size(DP), 1, experts), F32),
        direct,
        prob,
        soft,
        sums,
        name="first_col",
    )
    first_col = lax.all_to_all(partial_col, DP, 0, 0, tiled=True)
    second, first = call(
        functools.partial(second_kernel, ratio=ratio, tokens=tokens),
        (kept(whole, F32), kept(whole, F32)),
        gathered,
        gains,
        sums,
        flops=40 * all_tokens * experts,
        nbytes=10 * all_tokens * experts,
        name="second",
    )

    parts = 2 * across
    score, products = call(
        functools.partial(score_kernel, ratio=ratio),
        (
            kept(whole, BF16),
            jax.ShapeDtypeStruct((parts, along * rows, experts), BF16),
        ),
        second,
        first,
        gains,
        first_col,
        transposed,
        far=(4,),
        in_specs=[vmem] * 4 + [pl.BlockSpec(memory_space=pl.ANY)],
        out_specs=(vmem, vmem),
        scratch_shapes=[
            pltpu.VMEM((width, all_tokens), BF16),
            pltpu.SemaphoreType.DMA((parts,)),
        ],
        flops=2 * all_tokens * width * experts,
        nbytes=2 * all_tokens * width,
        name="score",
    )
    near = lax.all_to_all(products, ("y", "c"), 0, 0, tiled=True)
    far = call(
        functools.partial(near_kernel, along=along, rows=rows),
        jax.ShapeDtypeStruct((along, rows, experts), BF16),
        near,
        name="near",
    )
    far = lax.all_to_all(far, "z", 0, 0, tiled=True)

    chunk = 256 if width % 256 == 0 else width
    hidden_grad = call(
        functools.partial(hidden_kernel, rows=rows),
        jax.ShapeDtypeStruct((all_tokens, width), BF16),
        lax.axis_index("c").astype(jnp.int32)[None],
        score,
        across_parts,
        other_router,
        far=(0,),
        grid=(width // chunk,),
        in_specs=[
            pl.BlockSpec(memory_space=pltpu.SMEM),
            vmem,
            vmem,
            vmem,
        ],
        out_specs=pl.BlockSpec((all_tokens, chunk), lambda i: (0, i)),
        scratch_shapes=[pltpu.VMEM((width, experts), BF16)],
        flops=2 * all_tokens * width * experts,
        nbytes=2 * all_tokens * width,
        name="hidden_grad",
    )
    weight_grad = call(
        far_kernel, jax.ShapeDtypeStruct((rows, experts), F32), far, name="weight_grad"
    )
    return weight_grad, hidden_grad


def solution(mesh):
    dp, mp = mesh.devices.shape
    along = dp // 8
    split = Mesh(mesh.devices.reshape(4, along, 2, mp), ("y", "z", "c", "x"))
    token_rows = ("y", "z", "c", "x")
    weight_rows = ("x", "y", "z", "c")
    return jax.shard_map(
        body,
        mesh=split,
        in_specs=(
            P(DP, "x"),
            P(weight_rows, None),
            P(token_rows, None),
            P(),
            P(),
            P(token_rows),
            P(token_rows),
        ),
        out_specs=(P(weight_rows, None), P(DP, "x")),
        check_vma=False,
    )
```

```python
import functools

import jax
import jax.numpy as jnp
from jax import lax
from jax.experimental import pallas as pl
from jax.experimental.pallas import tpu as pltpu
from jax.sharding import Mesh
from jax.sharding import PartitionSpec as P

DP = ("y", "z", "c")
F32 = jnp.float32
BF16 = jnp.bfloat16
PAD = 16


def kept(shape, dtype):
    return pltpu.VMEM(shape, dtype)


def placed(array, near):
    return pltpu.with_memory_space_constraint(array, pltpu.VMEM if near else pltpu.HBM)


def call(kernel, shapes, *args, far=(), flops=0, nbytes=0, limit=16, name=None, **kwargs):
    return pl.pallas_call(
        kernel,
        out_shape=shapes,
        cost_estimate=pl.CostEstimate(flops=flops, transcendentals=0, bytes_accessed=nbytes),
        name=name,
        compiler_params=pltpu.CompilerParams(vmem_limit_bytes=limit << 20),
        **kwargs,
    )(*(placed(arg, at not in far) for at, arg in enumerate(args)))


def split_two(value):
    high = value.astype(BF16)
    low = (value - high.astype(F32)).astype(BF16)
    return high.astype(F32), low.astype(F32)


def as_column(row, tokens):
    shape = (tokens, row.shape[1])
    same = lax.broadcasted_iota(jnp.int32, shape, 0) == lax.broadcasted_iota(jnp.int32, shape, 1)
    return jnp.sum(jnp.where(same, row, 0.0), axis=1, keepdims=True)


def exponent_kernel(
    logits_ref, index_ref, grad_ref, first_ref, second_ref, router_ref, out_ref, gains_ref, sent_ref
):
    tokens, experts = logits_ref.shape
    logits = logits_ref[...]
    weight = jnp.exp(logits - jnp.max(logits, axis=1, keepdims=True))
    index = as_column(index_ref[...].astype(F32), tokens)
    hit = lax.broadcasted_iota(jnp.int32, (tokens, experts), 1).astype(F32) == index
    signed = jnp.where(hit, -weight, weight).astype(BF16)
    out_ref[:tokens, :] = signed
    high, low = split_two(grad_ref[...])
    rows = out_ref.shape[0] - tokens
    out_ref[tokens:, :] = jnp.zeros((rows, experts), BF16)
    row = lax.broadcasted_iota(jnp.int32, (rows, tokens), 0)
    tail = jnp.where(row == 0, high, jnp.where(row == 1, low, 0.0))
    out_ref[tokens:, :tokens] = tail.astype(BF16)
    first_gain = jnp.exp(first_ref[...])
    second_gain = jnp.exp(second_ref[...])
    gains_ref[0:1, :] = first_gain
    gains_ref[1:2, :] = second_gain
    weight = jnp.abs(signed.astype(F32))
    scale = as_column(high + low, tokens) / jnp.sum(weight * first_gain, axis=1, keepdims=True)
    total = jnp.sum(jnp.where(hit, weight * scale, 0.0), axis=0, keepdims=True)
    high, low = split_two(total * second_gain)
    rows = router_ref.shape[0]
    for member in range(sent_ref.shape[0]):
        sent_ref[member, :rows, :] = router_ref[...]
        sent_ref[member, rows : rows + 1, :] = high.astype(BF16)
        sent_ref[member, rows + 1 : rows + 2, :] = low.astype(BF16)


def tokens_of(gathered_ref, gains_ref, tokens):
    signed = gathered_ref[:tokens, :].astype(F32)
    tail = gathered_ref[tokens:, :].astype(F32)
    grad = as_column(tail[0:1, :] + tail[1:2, :], tokens)
    weight = jnp.abs(signed)
    second_scale = 1.0 / jnp.sum(weight * gains_ref[0:1, :], axis=1, keepdims=True)
    hot = jnp.where(signed < 0.0, grad, 0.0)
    return weight, second_scale, hot


def prepare_kernel(*refs, tokens, blocks):
    gains_ref, direct_ref, prob_ref, soft_ref = refs[blocks:]
    for block in range(blocks):
        weight, second_scale, hot = tokens_of(refs[block], gains_ref, tokens)
        here = slice(block * tokens, (block + 1) * tokens)
        prob = weight * gains_ref[1:2, :] * second_scale
        prob_ref[here, :] = prob
        direct_ref[here, :] = prob * hot
        soft_ref[here, :] = weight * gains_ref[0:1, :] * second_scale


def along_kernel(parts_ref, out_ref, *, rows):
    pair = parts_ref[:, rows : rows + 2, :].astype(F32)
    total = jnp.sum(jnp.sum(pair, axis=0), axis=0, keepdims=True)
    for member in range(out_ref.shape[0]):
        out_ref[member] = total


def second_row_grad(direct, prob, scaled):
    return jnp.sum(direct - prob * scaled, axis=1, keepdims=True)


def first_col_kernel(direct_ref, prob_ref, soft_ref, sums_ref, out_ref, *, ratio):
    scaled = ratio * jnp.sum(sums_ref[...], axis=0)
    row_grad = second_row_grad(direct_ref[...], prob_ref[...], scaled)
    total = -jnp.sum(soft_ref[...] * row_grad, axis=0, keepdims=True)
    for member in range(out_ref.shape[0]):
        out_ref[member] = total


def second_kernel(place_ref, *refs, ratio, tokens, blocks):
    gains_ref, sums_ref, out_ref, first_ref = refs[blocks:]
    scaled = ratio * jnp.sum(sums_ref[...], axis=0)
    for block in range(blocks):
        weight, second_scale, hot = tokens_of(refs[block], gains_ref, tokens)
        place = lax.rem(place_ref[0] + (blocks - block), blocks)
        here = pl.ds(pl.multiple_of(place * tokens, tokens), tokens)
        left = weight * second_scale * (gains_ref[1:2, :] * (hot - scaled))
        row = jnp.sum(left, axis=1, keepdims=True)
        out_ref[here, :] = left - weight * gains_ref[0:1, :] * (second_scale * row)
        first_ref[here, :] = weight * (1.0 / jnp.sum(weight, axis=1, keepdims=True))


def score_kernel(
    second_ref,
    first_ref,
    gains_ref,
    first_col_ref,
    hidden_ref,
    score_ref,
    out_ref,
    near_ref,
    done_ref,
    *,
    ratio,
):
    parts, size, _ = out_ref.shape
    copies = []
    for part in range(parts):
        here = pl.ds(part * size, size)
        copies.append(
            pltpu.make_async_copy(hidden_ref.at[here], near_ref.at[here], done_ref.at[part])
        )
        copies[part].start()
    scaled = ratio * gains_ref[0:1, :] * jnp.sum(first_col_ref[...], axis=0)
    first = first_ref[...]
    row = jnp.sum(first * scaled, axis=1, keepdims=True)
    score = (second_ref[...] - first * (scaled - row)).astype(BF16)
    score_ref[...] = score
    for part in range(parts):
        copies[part].wait()
        out_ref[part] = jnp.dot(
            near_ref[part * size : (part + 1) * size, :],
            score_ref[...],
            preferred_element_type=F32,
        ).astype(BF16)


def whole_part(value, size):
    return jnp.floor((value + 0.5) * (1.0 / size))


def transpose_kernel(hidden_ref, out_ref, *, along, rows):
    span = along * rows
    size = 4 * span if out_ref.shape[0] % (4 * span) == 0 else 2 * span
    target = lax.broadcasted_iota(jnp.int32, (size, size), 0).astype(F32)
    source = lax.broadcasted_iota(jnp.int32, (size, size), 1).astype(F32)
    outer = whole_part(target, 2 * span)
    rest = target - outer * (2 * span)
    core = whole_part(rest, span)
    rest = rest - core * span
    place = whole_part(rest, rows)
    wanted = outer * (2 * span) + place * (2 * rows) + core * rows + (rest - place * rows)
    order = jnp.where(source == wanted, 1.0, 0.0).astype(BF16)
    for start in range(0, out_ref.shape[0], size):
        out_ref[start : start + size, :] = lax.dot_general(
            order,
            hidden_ref[:, start : start + size],
            (((1,), (1,)), ((), ())),
            preferred_element_type=F32,
        ).astype(BF16)


def near_kernel(parts_ref, out_ref, *, along, rows):
    total = 0.0
    for member in range(parts_ref.shape[0]):
        total = total + parts_ref[member].astype(F32)
    for place in range(along):
        out_ref[place] = total[place * rows : (place + 1) * rows, :].astype(BF16)


def far_kernel(parts_ref, out_ref):
    total = 0.0
    for member in range(parts_ref.shape[0]):
        total = total + parts_ref[member].astype(F32)
    out_ref[...] = total


def hidden_kernel(place_ref, score_ref, mine_ref, other_ref, out_ref, router_ref, *, rows):
    members, padded, _ = mine_ref.shape
    along = padded // PAD
    size = 2 * along * rows

    @pl.when(pl.program_id(0) == 0)
    def _():
        target = lax.broadcasted_iota(jnp.int32, (size, padded), 0).astype(F32)
        column = lax.broadcasted_iota(jnp.int32, (size, padded), 1).astype(F32)
        place = whole_part(column, PAD)
        row = column - place * PAD
        base = place * (2 * rows) + row
        kept_row = row < rows
        mine_at = place_ref[0].astype(F32) * rows
        mine = jnp.where(kept_row & (target == base + mine_at), 1.0, 0.0).astype(BF16)
        other = jnp.where(kept_row & (target == base + (rows - mine_at)), 1.0, 0.0).astype(BF16)
        for member in range(members):
            whole = jnp.dot(mine, mine_ref[member], preferred_element_type=F32) + jnp.dot(
                other, other_ref[member], preferred_element_type=F32
            )
            at = lax.rem(place_ref[1] + (members - member), members)
            start = pl.multiple_of(at * size, size)
            router_ref[pl.ds(start, size), :] = whole.astype(BF16)

    width = out_ref.shape[1]
    start = pl.multiple_of(pl.program_id(0) * width, width)
    out_ref[...] = lax.dot_general(
        score_ref[...],
        router_ref[pl.ds(start, width), :],
        (((1,), (1,)), ((), ())),
        preferred_element_type=F32,
    ).astype(BF16)


def ahead(array, axis, step):
    size = lax.axis_size(axis)
    return lax.ppermute(array, axis, [(at, (at + step) % size) for at in range(size)])


def index_of(axis):
    return lax.axis_index(axis).astype(jnp.int32)


def body(hidden, router_weight, logits, first_pot, second_pot, expert_index, loss_grad):
    tokens, experts = logits.shape
    rows = router_weight.shape[0]
    across, along = lax.axis_size("y"), lax.axis_size("z")
    blocks = lax.axis_size("x")
    ratio = experts / (tokens * blocks * lax.axis_size(DP))
    all_tokens, width = hidden.shape
    vmem = pl.BlockSpec(memory_space=pltpu.VMEM)
    exponents, gains, sent = call(
        exponent_kernel,
        (
            kept((tokens + PAD, experts), BF16),
            kept((2, experts), F32),
            jax.ShapeDtypeStruct((along, PAD, experts), BF16),
        ),
        logits,
        expert_index[None],
        loss_grad[None],
        first_pot[None],
        second_pot[None],
        router_weight,
        far=range(6),
        name="exponents",
    )
    along_parts = lax.all_to_all(sent, "z", 0, 0, tiled=True)
    gathered = [exponents] + [ahead(exponents, "x", step) for step in range(1, blocks)]
    whole = (all_tokens, experts)

    transposed = call(
        functools.partial(transpose_kernel, along=along, rows=rows),
        jax.ShapeDtypeStruct((width, all_tokens), BF16),
        hidden,
        far=(0,),
        in_specs=[vmem],
        out_specs=vmem,
        flops=width * width * all_tokens,
        nbytes=4 * width * all_tokens,
        limit=32,
        name="transposed",
    )

    direct, prob, soft = call(
        functools.partial(prepare_kernel, tokens=tokens, blocks=blocks),
        (kept(whole, F32),) * 3,
        *gathered,
        gains,
        flops=40 * all_tokens * experts,
        nbytes=14 * all_tokens * experts,
        name="prepared",
    )
    sent = call(
        functools.partial(along_kernel, rows=rows),
        jax.ShapeDtypeStruct((2 * across * blocks, 1, experts), F32),
        along_parts,
        name="along",
    )
    sums = lax.all_to_all(sent, ("c", "y", "x"), 0, 0, tiled=True)
    mine = along_parts.reshape(1, along * PAD, experts)
    mine = jnp.concatenate([mine] + [ahead(mine, "y", step) for step in range(1, across)])

    partial_col = call(
        functools.partial(first_col_kernel, ratio=ratio),
        jax.ShapeDtypeStruct((lax.axis_size(DP), 1, experts), F32),
        direct,
        prob,
        soft,
        sums,
        name="first_col",
    )
    first_col = lax.all_to_all(partial_col, DP, 0, 0, tiled=True)
    second, first = call(
        functools.partial(second_kernel, ratio=ratio, tokens=tokens, blocks=blocks),
        (kept(whole, F32), kept(whole, F32)),
        index_of("x")[None],
        *gathered,
        gains,
        sums,
        flops=40 * all_tokens * experts,
        nbytes=10 * all_tokens * experts,
        in_specs=[pl.BlockSpec(memory_space=pltpu.SMEM)] + [vmem] * (blocks + 2),
        far=(0,),
        name="second",
    )

    second, mine = lax.optimization_barrier((second, mine))
    other = ahead(mine, "c", 1)
    parts = 2 * across
    score, products = call(
        functools.partial(score_kernel, ratio=ratio),
        (
            kept(whole, BF16),
            jax.ShapeDtypeStruct((parts, along * rows, experts), BF16),
        ),
        second,
        first,
        gains,
        first_col,
        transposed,
        far=(4,),
        in_specs=[vmem] * 4 + [pl.BlockSpec(memory_space=pl.ANY)],
        out_specs=(vmem, vmem),
        scratch_shapes=[
            pltpu.VMEM((width, all_tokens), BF16),
            pltpu.SemaphoreType.DMA((parts,)),
        ],
        flops=2 * all_tokens * width * experts,
        nbytes=2 * all_tokens * width,
        name="score",
    )
    near = lax.all_to_all(products, ("y", "c"), 0, 0, tiled=True)
    far = call(
        functools.partial(near_kernel, along=along, rows=rows),
        jax.ShapeDtypeStruct((along, rows, experts), BF16),
        near,
        name="near",
    )
    far = lax.all_to_all(far, "z", 0, 0, tiled=True)

    chunk = 256 if width % 256 == 0 else width
    hidden_grad = call(
        functools.partial(hidden_kernel, rows=rows),
        jax.ShapeDtypeStruct((all_tokens, width), BF16),
        jnp.stack([index_of("c"), index_of("y")]),
        score,
        mine,
        other,
        far=(0,),
        grid=(width // chunk,),
        in_specs=[
            pl.BlockSpec(memory_space=pltpu.SMEM),
            vmem,
            vmem,
            vmem,
        ],
        out_specs=pl.BlockSpec((all_tokens, chunk), lambda i: (0, i)),
        scratch_shapes=[pltpu.VMEM((width, experts), BF16)],
        flops=2 * all_tokens * width * experts,
        nbytes=2 * all_tokens * width,
        name="hidden_grad",
    )
    weight_grad = call(
        far_kernel, jax.ShapeDtypeStruct((rows, experts), F32), far, name="weight_grad"
    )
    return weight_grad, hidden_grad


def solution(mesh):
    dp, mp = mesh.devices.shape
    along = dp // 8
    split = Mesh(mesh.devices.reshape(4, along, 2, mp), ("y", "z", "c", "x"))
    token_rows = ("y", "z", "c", "x")
    weight_rows = ("x", "y", "z", "c")
    return jax.shard_map(
        body,
        mesh=split,
        in_specs=(
            P(DP, "x"),
            P(weight_rows, None),
            P(token_rows, None),
            P(),
            P(),
            P(token_rows),
            P(token_rows),
        ),
        out_specs=(P(weight_rows, None), P(DP, "x")),
        check_vma=False,
    )
```

```python
import functools

import jax
import jax.numpy as jnp
from jax import lax
from jax.experimental import pallas as pl
from jax.experimental.pallas import tpu as pltpu
from jax.sharding import Mesh
from jax.sharding import PartitionSpec as P

DP = ("y", "z", "c")
F32 = jnp.float32
BF16 = jnp.bfloat16
PAD = 16


def kept(shape, dtype):
    return pltpu.VMEM(shape, dtype)


def outside(shape, dtype):
    return pltpu.HBM(shape, dtype)


def placed(array, near):
    return pltpu.with_memory_space_constraint(array, pltpu.VMEM if near else pltpu.HBM)


def call(kernel, shapes, *args, far=(), flops=0, nbytes=0, limit=16, **kwargs):
    return pl.pallas_call(
        kernel,
        out_shape=shapes,
        cost_estimate=pl.CostEstimate(flops=flops, transcendentals=0, bytes_accessed=nbytes),
        compiler_params=pltpu.CompilerParams(vmem_limit_bytes=limit << 20),
        **kwargs,
    )(*(placed(arg, at not in far) for at, arg in enumerate(args)))


def split_two(value):
    high = value.astype(BF16)
    low = (value - high.astype(F32)).astype(BF16)
    return high.astype(F32), low.astype(F32)


def as_column(row, tokens):
    shape = (tokens, row.shape[1])
    same = lax.broadcasted_iota(jnp.int32, shape, 0) == lax.broadcasted_iota(jnp.int32, shape, 1)
    return jnp.sum(jnp.where(same, row, 0.0), axis=1, keepdims=True)


def exponent_kernel(
    logits_ref, index_ref, grad_ref, first_ref, second_ref, router_ref, out_ref, gains_ref, sent_ref
):
    tokens, experts = logits_ref.shape
    logits = logits_ref[...]
    weight = jnp.exp(logits - jnp.max(logits, axis=1, keepdims=True))
    index = as_column(index_ref[...].astype(F32), tokens)
    hit = lax.broadcasted_iota(jnp.int32, (tokens, experts), 1).astype(F32) == index
    signed = jnp.where(hit, -weight, weight).astype(BF16)
    out_ref[:tokens, :] = signed
    high, low = split_two(grad_ref[...])
    rows = out_ref.shape[0] - tokens
    out_ref[tokens:, :] = jnp.zeros((rows, experts), BF16)
    row = lax.broadcasted_iota(jnp.int32, (rows, tokens), 0)
    tail = jnp.where(row == 0, high, jnp.where(row == 1, low, 0.0))
    out_ref[tokens:, :tokens] = tail.astype(BF16)
    first_gain = jnp.exp(first_ref[...])
    second_gain = jnp.exp(second_ref[...])
    gains_ref[0:1, :] = first_gain
    gains_ref[1:2, :] = second_gain
    weight = jnp.abs(signed.astype(F32))
    scale = as_column(high + low, tokens) / jnp.sum(weight * first_gain, axis=1, keepdims=True)
    total = jnp.sum(jnp.where(hit, weight * scale, 0.0), axis=0, keepdims=True)
    high, low = split_two(total * second_gain)
    rows = router_ref.shape[0]
    for member in range(sent_ref.shape[0]):
        sent_ref[member, :rows, :] = router_ref[...]
        sent_ref[member, rows : rows + 1, :] = high.astype(BF16)
        sent_ref[member, rows + 1 : rows + 2, :] = low.astype(BF16)


def tokens_of(gathered_ref, gains_ref, block, tokens):
    signed = gathered_ref[block, :tokens, :].astype(F32)
    tail = gathered_ref[block, tokens:, :].astype(F32)
    grad = as_column(tail[0:1, :] + tail[1:2, :], tokens)
    weight = jnp.abs(signed)
    second_scale = 1.0 / jnp.sum(weight * gains_ref[0:1, :], axis=1, keepdims=True)
    hot = jnp.where(signed < 0.0, grad, 0.0)
    return weight, second_scale, hot


def along_kernel(parts_ref, out_ref, *, rows):
    pair = parts_ref[:, rows : rows + 2, :].astype(F32)
    total = jnp.sum(jnp.sum(pair, axis=0), axis=0, keepdims=True)
    high, low = split_two(total)
    block = parts_ref[0].astype(F32)
    row = lax.broadcasted_iota(jnp.int32, block.shape, 0)
    block = jnp.where(row == rows, high, jnp.where(row == rows + 1, low, block)).astype(BF16)
    for copy in range(out_ref.shape[0]):
        out_ref[copy, 0:PAD, :] = block
        for member in range(1, parts_ref.shape[0]):
            out_ref[copy, member * PAD : (member + 1) * PAD, :] = parts_ref[member]


def across_kernel(parts_ref, exponents_ref, out_ref, *, rows, tokens):
    total = 0.0
    for member in range(parts_ref.shape[0]):
        block = parts_ref[member, 0:PAD, :].astype(F32)
        total = total + jnp.sum(block[rows : rows + 2, :], axis=0, keepdims=True)
    high, low = split_two(total)
    tail = exponents_ref[tokens:, :].astype(F32)
    row = lax.broadcasted_iota(jnp.int32, tail.shape, 0)
    tail = jnp.where(row == 2, high, jnp.where(row == 3, low, tail)).astype(BF16)
    for copy in range(out_ref.shape[0]):
        out_ref[copy, :tokens, :] = exponents_ref[:tokens, :]
        out_ref[copy, tokens:, :] = tail


def column_sum(gathered_ref, tokens):
    total = 0.0
    for block in range(gathered_ref.shape[0]):
        tail = gathered_ref[block, tokens:, :].astype(F32)
        total = total + jnp.sum(tail[2:4, :], axis=0, keepdims=True)
    return total


def first_col_kernel(gathered_ref, gains_ref, out_ref, *, ratio, tokens):
    scaled = ratio * column_sum(gathered_ref, tokens)
    total = 0.0
    for block in range(gathered_ref.shape[0]):
        weight, second_scale, hot = tokens_of(gathered_ref, gains_ref, block, tokens)
        left = weight * (gains_ref[1:2, :] * (hot - scaled))
        row = jnp.sum(left, axis=1, keepdims=True)
        total = total - jnp.sum(
            weight * (row * second_scale * second_scale), axis=0, keepdims=True
        )
    total = total * gains_ref[0:1, :]
    for member in range(out_ref.shape[0]):
        out_ref[member] = total


def sum_kernel(parts_ref, out_ref):
    total = jnp.sum(parts_ref[...], axis=0)
    for copy in range(out_ref.shape[0]):
        out_ref[copy] = total


def score_kernel(
    core_ref,
    gathered_ref,
    gains_ref,
    first_col_ref,
    mine_ref,
    other_ref,
    score_ref,
    out_ref,
    near_ref,
    half_ref,
    made_ref,
    half_done_ref,
    score_sent_ref,
    sent_ref,
    *,
    ratio,
    tokens,
):
    half_copy = pltpu.make_async_copy(other_ref, half_ref, half_done_ref)
    half_copy.start()
    scaled = ratio * column_sum(gathered_ref, tokens)
    first_scaled = ratio * gains_ref[0:1, :] * jnp.sum(first_col_ref[...], axis=0)
    blocks = gathered_ref.shape[0] // 2
    for side in range(2):
        start = (core_ref[0] * (1 - side) + (1 - core_ref[0]) * side) * blocks
        for block in range(blocks):
            weight, second_scale, hot = tokens_of(gathered_ref, gains_ref, start + block, tokens)
            left = second_scale * (gains_ref[1:2, :] * (hot - scaled))
            row = jnp.sum(weight * left, axis=1, keepdims=True)
            left = left - gains_ref[0:1, :] * (second_scale * row)
            first_scale = 1.0 / jnp.sum(weight, axis=1, keepdims=True)
            row = jnp.sum(weight * first_scaled, axis=1, keepdims=True) * first_scale
            score = weight * (left - first_scale * (first_scaled - row))
            near_ref[side, block * tokens : (block + 1) * tokens, :] = score.astype(BF16)
    score_copy = pltpu.make_async_copy(near_ref.at[0], score_ref, score_sent_ref)
    score_copy.start()
    half_copy.wait()
    parts = made_ref.shape[0]
    copies = []
    for part in range(parts):
        made_ref[part] = (
            jnp.dot(mine_ref[part], near_ref[0], preferred_element_type=F32)
            + jnp.dot(half_ref[part], near_ref[1], preferred_element_type=F32)
        ).astype(BF16)
        copies.append(
            pltpu.make_async_copy(made_ref.at[part], out_ref.at[part], sent_ref.at[part])
        )
        copies[part].start()
    score_copy.wait()
    for part in range(parts):
        copies[part].wait()


def whole_part(value, size):
    return jnp.floor((value + 0.5) * (1.0 / size))


def transpose_kernel(core_ref, hidden_ref, mine_ref, other_ref, *, along, rows):
    span = along * rows
    whole = hidden_ref.shape[1]
    mine = core_ref[0].astype(F32)
    orders = {}
    for member in range(whole // (2 * span)):
        start = member * 2 * span
        first = start // 128 * 128
        last = min(-(-(start + 2 * span) // 128) * 128, whole)
        key = (start - first, last - first)
        if key not in orders:
            target = lax.broadcasted_iota(jnp.int32, (2 * span, 128), 0).astype(F32)[:, 0:1]
            side = whole_part(target, span)
            core = mine + side * (1.0 - 2.0 * mine)
            rest = target - side * span
            place = whole_part(rest, rows)
            wanted = place * (2 * rows) + core * rows + (rest - place * rows) + key[0]
            source = lax.broadcasted_iota(jnp.int32, (2 * span, key[1]), 1).astype(F32)
            orders[key] = jnp.where(source == wanted, 1.0, 0.0).astype(BF16)
        both = lax.dot_general(
            orders[key],
            hidden_ref[:, first:last],
            (((1,), (1,)), ((), ())),
            preferred_element_type=F32,
        ).astype(BF16)
        mine_ref[member] = both[:span]
        other_ref[member] = both[span:]


def near_kernel(parts_ref, out_ref, *, along, rows):
    total = 0.0
    for member in range(parts_ref.shape[0]):
        total = total + parts_ref[member].astype(F32)
    for place in range(along):
        out_ref[place] = total[place * rows : (place + 1) * rows, :].astype(BF16)


def far_kernel(parts_ref, out_ref):
    total = 0.0
    for member in range(parts_ref.shape[0]):
        total = total + parts_ref[member].astype(F32)
    out_ref[...] = total


def hidden_kernel(place_ref, score_ref, mine_ref, other_ref, out_ref, router_ref, *, rows):
    members, padded, _ = mine_ref.shape
    along = padded // PAD
    size = 2 * along * rows

    @pl.when(pl.program_id(0) == 0)
    def _():
        target = lax.broadcasted_iota(jnp.int32, (size, padded), 0).astype(F32)
        column = lax.broadcasted_iota(jnp.int32, (size, padded), 1).astype(F32)
        place = whole_part(column, PAD)
        row = column - place * PAD
        base = place * (2 * rows) + row
        kept_row = row < rows
        mine_at = place_ref[0].astype(F32) * rows
        mine = jnp.where(kept_row & (target == base + mine_at), 1.0, 0.0).astype(BF16)
        other = jnp.where(kept_row & (target == base + (rows - mine_at)), 1.0, 0.0).astype(BF16)
        for member in range(members):
            whole = jnp.dot(mine, mine_ref[member], preferred_element_type=F32) + jnp.dot(
                other, other_ref[member], preferred_element_type=F32
            )
            router_ref[member * size : (member + 1) * size, :] = whole.astype(BF16)

    width = out_ref.shape[1]
    start = pl.multiple_of(pl.program_id(0) * width, width)
    out_ref[...] = lax.dot_general(
        score_ref[...],
        router_ref[pl.ds(start, width), :],
        (((1,), (1,)), ((), ())),
        preferred_element_type=F32,
    ).astype(BF16)


def ahead(array, axis, step):
    size = lax.axis_size(axis)
    return lax.ppermute(array, axis, [(at, (at + step) % size) for at in range(size)])


def index_of(axis):
    return lax.axis_index(axis).astype(jnp.int32)


def body(hidden, router_weight, logits, first_pot, second_pot, expert_index, loss_grad):
    tokens, experts = logits.shape
    rows = router_weight.shape[0]
    across, along = lax.axis_size("y"), lax.axis_size("z")
    blocks = lax.axis_size("x")
    ratio = experts / (tokens * blocks * lax.axis_size(DP))
    all_tokens, width = hidden.shape
    vmem = pl.BlockSpec(memory_space=pltpu.VMEM)
    exponents, gains, sent = call(
        exponent_kernel,
        (
            kept((tokens + PAD, experts), BF16),
            kept((2, experts), F32),
            jax.ShapeDtypeStruct((along, PAD, experts), BF16),
        ),
        logits,
        expert_index[None],
        loss_grad[None],
        first_pot[None],
        second_pot[None],
        router_weight,
        far=range(6),
    )
    sent, core = lax.optimization_barrier((sent, index_of("c")[None]))
    along_parts = lax.all_to_all(sent, "z", 0, 0, tiled=True)
    along_parts, hidden = lax.optimization_barrier((along_parts, hidden))
    whole = (all_tokens, experts)

    half = (across, along * rows, all_tokens)
    smem = pl.BlockSpec(memory_space=pltpu.SMEM)
    transposed, other_half = call(
        functools.partial(transpose_kernel, along=along, rows=rows),
        (kept(half, BF16), outside(half, BF16)),
        core,
        hidden,
        far=(0, 1),
        in_specs=[smem, vmem],
        out_specs=(vmem, vmem),
        flops=width * width * all_tokens,
        nbytes=4 * width * all_tokens,
        limit=32,
    )
    other_half = ahead(other_half, "c", 1)
    sent = call(
        functools.partial(along_kernel, rows=rows),
        kept((across, along * PAD, experts), BF16),
        along_parts,
    )
    across_parts = lax.all_to_all(sent, "y", 0, 0, tiled=True)
    across_parts, transposed = lax.optimization_barrier((across_parts, transposed))
    sent = call(
        functools.partial(across_kernel, rows=rows, tokens=tokens),
        kept((blocks, tokens + PAD, experts), BF16),
        across_parts,
        exponents,
    )
    gathered = lax.all_to_all(sent, "x", 0, 0, tiled=True)
    gathered = lax.all_gather(gathered, "c", tiled=True)
    gathered, other_half = lax.optimization_barrier((gathered, other_half))
    partial_col = call(
        functools.partial(first_col_kernel, ratio=ratio, tokens=tokens),
        kept((along, 1, experts), F32),
        gathered,
        gains,
    )
    partial_col = call(
        sum_kernel,
        kept((across, 1, experts), F32),
        lax.all_to_all(partial_col, "z", 0, 0, tiled=True),
    )
    first_col = lax.all_to_all(partial_col, "y", 0, 0, tiled=True)

    made = (across, along * rows, experts)
    score, products = call(
        functools.partial(score_kernel, ratio=ratio, tokens=tokens),
        (outside(whole, BF16), outside(made, BF16)),
        core,
        gathered,
        gains,
        first_col,
        transposed,
        other_half,
        far=(0, 5),
        in_specs=[smem] + [vmem] * 4 + [pl.BlockSpec(memory_space=pl.ANY)],
        out_specs=(pl.BlockSpec(memory_space=pl.ANY),) * 2,
        scratch_shapes=[
            pltpu.VMEM((2, *whole), BF16),
            pltpu.VMEM(half, BF16),
            pltpu.VMEM(made, BF16),
            pltpu.SemaphoreType.DMA,
            pltpu.SemaphoreType.DMA,
            pltpu.SemaphoreType.DMA((across,)),
        ],
        flops=2 * all_tokens * width * experts,
        nbytes=2 * all_tokens * width,
    )
    score, mine = lax.optimization_barrier((score, across_parts))
    other = ahead(mine, "c", 1)
    near = lax.all_to_all(products, "y", 0, 0, tiled=True)
    far = call(
        functools.partial(near_kernel, along=along, rows=rows),
        jax.ShapeDtypeStruct((along, rows, experts), BF16),
        near,
    )
    chunk = 896 if width % 896 == 0 else width
    hidden_grad = call(
        functools.partial(hidden_kernel, rows=rows),
        jax.ShapeDtypeStruct((all_tokens, width), BF16),
        core,
        score,
        mine,
        other,
        far=(0, 1),
        grid=(width // chunk,),
        in_specs=[
            pl.BlockSpec(memory_space=pltpu.SMEM),
            vmem,
            vmem,
            vmem,
        ],
        out_specs=pl.BlockSpec((all_tokens, chunk), lambda i: (0, i)),
        scratch_shapes=[pltpu.VMEM((width, experts), BF16)],
        flops=2 * all_tokens * width * experts,
        nbytes=2 * all_tokens * width,
    )
    far, hidden_grad = lax.optimization_barrier((far, hidden_grad))
    far = lax.all_to_all(far, "z", 0, 0, tiled=True)
    weight_grad = call(far_kernel, jax.ShapeDtypeStruct((rows, experts), F32), far)
    return weight_grad, hidden_grad


def solution(mesh):
    dp, mp = mesh.devices.shape
    along = dp // 8
    split = Mesh(mesh.devices.reshape(4, along, 2, mp), ("y", "z", "c", "x"))
    token_rows = ("y", "z", "c", "x")
    weight_rows = ("x", "y", "z", "c")

    return jax.shard_map(
        body,
        mesh=split,
        in_specs=(
            P(DP, "x"),
            P(weight_rows, None),
            P(token_rows, None),
            P(),
            P(),
            P(token_rows),
            P(token_rows),
        ),
        out_specs=(P(weight_rows, None), P(DP, "x")),
        check_vma=False,
    )
```

```python
import functools

import jax
import jax.numpy as jnp
from jax import lax
from jax.experimental import pallas as pl
from jax.experimental.pallas import tpu as pltpu
from jax.sharding import Mesh
from jax.sharding import PartitionSpec as P

DP = ("y", "z", "c")
F32 = jnp.float32
BF16 = jnp.bfloat16
PAD = 16


def kept(shape, dtype):
    return pltpu.VMEM(shape, dtype)


def outside(shape, dtype):
    return pltpu.HBM(shape, dtype)


def placed(array, near):
    return pltpu.with_memory_space_constraint(array, pltpu.VMEM if near else pltpu.HBM)


def call(kernel, shapes, *args, far=(), flops=0, nbytes=0, limit=16, **kwargs):
    return pl.pallas_call(
        kernel,
        out_shape=shapes,
        cost_estimate=pl.CostEstimate(flops=flops, transcendentals=0, bytes_accessed=nbytes),
        compiler_params=pltpu.CompilerParams(vmem_limit_bytes=limit << 20),
        **kwargs,
    )(*(placed(arg, at not in far) for at, arg in enumerate(args)))


def split_two(value):
    high = value.astype(BF16)
    low = (value - high.astype(F32)).astype(BF16)
    return high.astype(F32), low.astype(F32)


def as_column(row, tokens):
    shape = (tokens, row.shape[1])
    same = lax.broadcasted_iota(jnp.int32, shape, 0) == lax.broadcasted_iota(jnp.int32, shape, 1)
    return jnp.sum(jnp.where(same, row, 0.0), axis=1, keepdims=True)


def exponent_kernel(
    logits_ref, index_ref, grad_ref, first_ref, second_ref, router_ref, out_ref, gains_ref, sent_ref
):
    tokens, experts = logits_ref.shape
    logits = logits_ref[...]
    weight = jnp.exp(logits - jnp.max(logits, axis=1, keepdims=True))
    index = as_column(index_ref[...].astype(F32), tokens)
    hit = lax.broadcasted_iota(jnp.int32, (tokens, experts), 1).astype(F32) == index
    signed = jnp.where(hit, -weight, weight).astype(BF16)
    out_ref[:tokens, :] = signed
    high, low = split_two(grad_ref[...])
    rows = out_ref.shape[0] - tokens
    out_ref[tokens:, :] = jnp.zeros((rows, experts), BF16)
    row = lax.broadcasted_iota(jnp.int32, (rows, tokens), 0)
    tail = jnp.where(row == 0, high, jnp.where(row == 1, low, 0.0))
    out_ref[tokens:, :tokens] = tail.astype(BF16)
    first_gain = jnp.exp(first_ref[...])
    second_gain = jnp.exp(second_ref[...])
    gains_ref[0:1, :] = first_gain
    gains_ref[1:2, :] = second_gain
    weight = jnp.abs(signed.astype(F32))
    scale = as_column(high + low, tokens) / jnp.sum(weight * first_gain, axis=1, keepdims=True)
    total = jnp.sum(jnp.where(hit, weight * scale, 0.0), axis=0, keepdims=True)
    high, low = split_two(total * second_gain)
    rows = router_ref.shape[0]
    for member in range(sent_ref.shape[0]):
        sent_ref[member, :rows, :] = router_ref[...]
        sent_ref[member, rows : rows + 1, :] = high.astype(BF16)
        sent_ref[member, rows + 1 : rows + 2, :] = low.astype(BF16)


def tokens_of(gathered_ref, gains_ref, block, tokens):
    signed = gathered_ref[block, :tokens, :].astype(F32)
    tail = gathered_ref[block, tokens:, :].astype(F32)
    grad = as_column(tail[0:1, :] + tail[1:2, :], tokens)
    weight = jnp.abs(signed)
    second_scale = 1.0 / jnp.sum(weight * gains_ref[0:1, :], axis=1, keepdims=True)
    hot = jnp.where(signed < 0.0, grad, 0.0)
    return weight, second_scale, hot


def along_kernel(parts_ref, out_ref, *, rows):
    pair = parts_ref[:, rows : rows + 2, :].astype(F32)
    total = jnp.sum(jnp.sum(pair, axis=0), axis=0, keepdims=True)
    high, low = split_two(total)
    block = parts_ref[0].astype(F32)
    row = lax.broadcasted_iota(jnp.int32, block.shape, 0)
    block = jnp.where(row == rows, high, jnp.where(row == rows + 1, low, block)).astype(BF16)
    for copy in range(out_ref.shape[0]):
        out_ref[copy, 0:PAD, :] = block
        for member in range(1, parts_ref.shape[0]):
            out_ref[copy, member * PAD : (member + 1) * PAD, :] = parts_ref[member]


def across_kernel(parts_ref, exponents_ref, out_ref, *, rows, tokens):
    total = 0.0
    for member in range(parts_ref.shape[0]):
        block = parts_ref[member, 0:PAD, :].astype(F32)
        total = total + jnp.sum(block[rows : rows + 2, :], axis=0, keepdims=True)
    high, low = split_two(total)
    tail = exponents_ref[tokens:, :].astype(F32)
    row = lax.broadcasted_iota(jnp.int32, tail.shape, 0)
    tail = jnp.where(row == 2, high, jnp.where(row == 3, low, tail)).astype(BF16)
    for copy in range(out_ref.shape[0]):
        out_ref[copy, :tokens, :] = exponents_ref[:tokens, :]
        out_ref[copy, tokens:, :] = tail


def column_sum(gathered_ref, tokens):
    total = 0.0
    for block in range(gathered_ref.shape[0]):
        tail = gathered_ref[block, tokens:, :].astype(F32)
        total = total + jnp.sum(tail[2:4, :], axis=0, keepdims=True)
    return total


def first_col_kernel(gathered_ref, gains_ref, out_ref, *, ratio, tokens):
    scaled = ratio * column_sum(gathered_ref, tokens)
    total = 0.0
    for block in range(gathered_ref.shape[0]):
        weight, second_scale, hot = tokens_of(gathered_ref, gains_ref, block, tokens)
        left = weight * (gains_ref[1:2, :] * (hot - scaled))
        row = jnp.sum(left, axis=1, keepdims=True)
        total = total - jnp.sum(
            weight * (row * second_scale * second_scale), axis=0, keepdims=True
        )
    total = total * gains_ref[0:1, :]
    for member in range(out_ref.shape[0]):
        out_ref[member] = total


def score_kernel(
    core_ref,
    gathered_ref,
    gains_ref,
    first_col_ref,
    mine_ref,
    other_ref,
    score_ref,
    out_ref,
    near_ref,
    half_ref,
    made_ref,
    half_done_ref,
    score_sent_ref,
    sent_ref,
    *,
    ratio,
    tokens,
):
    half_copy = pltpu.make_async_copy(other_ref, half_ref, half_done_ref)
    half_copy.start()
    scaled = ratio * column_sum(gathered_ref, tokens)
    first_scaled = ratio * gains_ref[0:1, :] * jnp.sum(first_col_ref[...], axis=0)
    blocks = gathered_ref.shape[0] // 2
    for side in range(2):
        start = (core_ref[0] * (1 - side) + (1 - core_ref[0]) * side) * blocks
        for block in range(blocks):
            weight, second_scale, hot = tokens_of(gathered_ref, gains_ref, start + block, tokens)
            left = second_scale * (gains_ref[1:2, :] * (hot - scaled))
            row = jnp.sum(weight * left, axis=1, keepdims=True)
            left = left - gains_ref[0:1, :] * (second_scale * row)
            first_scale = 1.0 / jnp.sum(weight, axis=1, keepdims=True)
            row = jnp.sum(weight * first_scaled, axis=1, keepdims=True) * first_scale
            score = weight * (left - first_scale * (first_scaled - row))
            near_ref[side, block * tokens : (block + 1) * tokens, :] = score.astype(BF16)
    score_copy = pltpu.make_async_copy(near_ref.at[0], score_ref, score_sent_ref)
    score_copy.start()
    half_copy.wait()
    parts = made_ref.shape[0]
    copies = []
    for part in range(parts):
        made_ref[part] = (
            jnp.dot(mine_ref[part], near_ref[0], preferred_element_type=F32)
            + jnp.dot(half_ref[part], near_ref[1], preferred_element_type=F32)
        ).astype(BF16)
        copies.append(
            pltpu.make_async_copy(made_ref.at[part], out_ref.at[part], sent_ref.at[part])
        )
        copies[part].start()
    score_copy.wait()
    for part in range(parts):
        copies[part].wait()


def whole_part(value, size):
    return jnp.floor((value + 0.5) * (1.0 / size))


def transpose_kernel(core_ref, hidden_ref, mine_ref, other_ref, *, along, rows):
    span = along * rows
    whole = hidden_ref.shape[1]
    mine = core_ref[0].astype(F32)
    orders = {}
    for member in range(whole // (2 * span)):
        start = member * 2 * span
        first = start // 128 * 128
        last = min(-(-(start + 2 * span) // 128) * 128, whole)
        key = (start - first, last - first)
        if key not in orders:
            target = lax.broadcasted_iota(jnp.int32, (2 * span, 128), 0).astype(F32)[:, 0:1]
            side = whole_part(target, span)
            core = mine + side * (1.0 - 2.0 * mine)
            rest = target - side * span
            place = whole_part(rest, rows)
            wanted = place * (2 * rows) + core * rows + (rest - place * rows) + key[0]
            source = lax.broadcasted_iota(jnp.int32, (2 * span, key[1]), 1).astype(F32)
            orders[key] = jnp.where(source == wanted, 1.0, 0.0).astype(BF16)
        both = lax.dot_general(
            orders[key],
            hidden_ref[:, first:last],
            (((1,), (1,)), ((), ())),
            preferred_element_type=F32,
        ).astype(BF16)
        mine_ref[member] = both[:span]
        other_ref[member] = both[span:]


def near_kernel(parts_ref, out_ref, *, along, rows):
    total = 0.0
    for member in range(parts_ref.shape[0]):
        total = total + parts_ref[member].astype(F32)
    for place in range(along):
        out_ref[place] = total[place * rows : (place + 1) * rows, :].astype(BF16)


def far_kernel(parts_ref, out_ref):
    total = 0.0
    for member in range(parts_ref.shape[0]):
        total = total + parts_ref[member].astype(F32)
    out_ref[...] = total


def hidden_kernel(place_ref, score_ref, mine_ref, other_ref, out_ref, router_ref, *, rows):
    members, padded, _ = mine_ref.shape
    along = padded // PAD
    size = 2 * along * rows

    @pl.when(pl.program_id(0) == 0)
    def _():
        target = lax.broadcasted_iota(jnp.int32, (size, padded), 0).astype(F32)
        column = lax.broadcasted_iota(jnp.int32, (size, padded), 1).astype(F32)
        place = whole_part(column, PAD)
        row = column - place * PAD
        base = place * (2 * rows) + row
        kept_row = row < rows
        mine_at = place_ref[0].astype(F32) * rows
        mine = jnp.where(kept_row & (target == base + mine_at), 1.0, 0.0).astype(BF16)
        other = jnp.where(kept_row & (target == base + (rows - mine_at)), 1.0, 0.0).astype(BF16)
        for member in range(members):
            whole = jnp.dot(mine, mine_ref[member], preferred_element_type=F32) + jnp.dot(
                other, other_ref[member], preferred_element_type=F32
            )
            router_ref[member * size : (member + 1) * size, :] = whole.astype(BF16)

    width = out_ref.shape[1]
    start = pl.multiple_of(pl.program_id(0) * width, width)
    out_ref[...] = lax.dot_general(
        score_ref[...],
        router_ref[pl.ds(start, width), :],
        (((1,), (1,)), ((), ())),
        preferred_element_type=F32,
    ).astype(BF16)


def ahead(array, axis, step):
    size = lax.axis_size(axis)
    return lax.ppermute(array, axis, [(at, (at + step) % size) for at in range(size)])


def index_of(axis):
    return lax.axis_index(axis).astype(jnp.int32)


def body(hidden, router_weight, logits, first_pot, second_pot, expert_index, loss_grad):
    tokens, experts = logits.shape
    rows = router_weight.shape[0]
    across, along = lax.axis_size("y"), lax.axis_size("z")
    blocks = lax.axis_size("x")
    ratio = experts / (tokens * blocks * lax.axis_size(DP))
    all_tokens, width = hidden.shape
    vmem = pl.BlockSpec(memory_space=pltpu.VMEM)
    exponents, gains, sent = call(
        exponent_kernel,
        (
            kept((tokens + PAD, experts), BF16),
            kept((2, experts), F32),
            jax.ShapeDtypeStruct((along, PAD, experts), BF16),
        ),
        logits,
        expert_index[None],
        loss_grad[None],
        first_pot[None],
        second_pot[None],
        router_weight,
        far=range(6),
    )
    sent, core = lax.optimization_barrier((sent, index_of("c")[None]))
    along_parts = lax.all_to_all(sent, "z", 0, 0, tiled=True)
    along_parts, hidden = lax.optimization_barrier((along_parts, hidden))
    whole = (all_tokens, experts)

    half = (across, along * rows, all_tokens)
    smem = pl.BlockSpec(memory_space=pltpu.SMEM)
    transposed, other_half = call(
        functools.partial(transpose_kernel, along=along, rows=rows),
        (kept(half, BF16), outside(half, BF16)),
        core,
        hidden,
        far=(0, 1),
        in_specs=[smem, vmem],
        out_specs=(vmem, vmem),
        flops=width * width * all_tokens,
        nbytes=4 * width * all_tokens,
        limit=32,
    )
    other_half = ahead(other_half, "c", 1)
    sent = call(
        functools.partial(along_kernel, rows=rows),
        kept((across, along * PAD, experts), BF16),
        along_parts,
    )
    across_parts = lax.all_to_all(sent, "y", 0, 0, tiled=True)
    across_parts, transposed = lax.optimization_barrier((across_parts, transposed))
    sent = call(
        functools.partial(across_kernel, rows=rows, tokens=tokens),
        kept((blocks, tokens + PAD, experts), BF16),
        across_parts,
        exponents,
    )
    gathered = lax.all_to_all(sent, "x", 0, 0, tiled=True)
    gathered = lax.all_gather(gathered, "c", tiled=True)
    gathered, other_half = lax.optimization_barrier((gathered, other_half))
    partial_col = call(
        functools.partial(first_col_kernel, ratio=ratio, tokens=tokens),
        kept((along * across, 1, experts), F32),
        gathered,
        gains,
    )
    first_col = lax.all_to_all(partial_col, ("z", "y"), 0, 0, tiled=True)

    made = (across, along * rows, experts)
    score, products = call(
        functools.partial(score_kernel, ratio=ratio, tokens=tokens),
        (outside(whole, BF16), outside(made, BF16)),
        core,
        gathered,
        gains,
        first_col,
        transposed,
        other_half,
        far=(0, 5),
        in_specs=[smem] + [vmem] * 4 + [pl.BlockSpec(memory_space=pl.ANY)],
        out_specs=(pl.BlockSpec(memory_space=pl.ANY),) * 2,
        scratch_shapes=[
            pltpu.VMEM((2, *whole), BF16),
            pltpu.VMEM(half, BF16),
            pltpu.VMEM(made, BF16),
            pltpu.SemaphoreType.DMA,
            pltpu.SemaphoreType.DMA,
            pltpu.SemaphoreType.DMA((across,)),
        ],
        flops=2 * all_tokens * width * experts,
        nbytes=2 * all_tokens * width,
    )
    score, mine = lax.optimization_barrier((score, across_parts))
    other = ahead(mine, "c", 1)
    near = lax.all_to_all(products, "y", 0, 0, tiled=True)
    far = call(
        functools.partial(near_kernel, along=along, rows=rows),
        jax.ShapeDtypeStruct((along, rows, experts), BF16),
        near,
    )
    chunk = 896 if width % 896 == 0 else width
    hidden_grad = call(
        functools.partial(hidden_kernel, rows=rows),
        jax.ShapeDtypeStruct((all_tokens, width), BF16),
        core,
        score,
        mine,
        other,
        far=(0, 1),
        grid=(width // chunk,),
        in_specs=[
            pl.BlockSpec(memory_space=pltpu.SMEM),
            vmem,
            vmem,
            vmem,
        ],
        out_specs=pl.BlockSpec((all_tokens, chunk), lambda i: (0, i)),
        scratch_shapes=[pltpu.VMEM((width, experts), BF16)],
        flops=2 * all_tokens * width * experts,
        nbytes=2 * all_tokens * width,
    )
    far, hidden_grad = lax.optimization_barrier((far, hidden_grad))
    far = lax.all_to_all(far, "z", 0, 0, tiled=True)
    weight_grad = call(far_kernel, jax.ShapeDtypeStruct((rows, experts), F32), far)
    return weight_grad, hidden_grad


def solution(mesh):
    dp, mp = mesh.devices.shape
    along = dp // 8
    split = Mesh(mesh.devices.reshape(4, along, 2, mp), ("y", "z", "c", "x"))
    token_rows = ("y", "z", "c", "x")
    weight_rows = ("x", "y", "z", "c")

    return jax.shard_map(
        body,
        mesh=split,
        in_specs=(
            P(DP, "x"),
            P(weight_rows, None),
            P(token_rows, None),
            P(),
            P(),
            P(token_rows),
            P(token_rows),
        ),
        out_specs=(P(weight_rows, None), P(DP, "x")),
        check_vma=False,
    )
```
